8 devices in a mesh: dp: 1 (over z), tp: 8 (over y, x, core).
Axes of the slice: x: 2, y: 2, z: 1, core: 2. Of those that a mesh axis runs over, the one named last changes fastest.
Arguments:
- x_steps: bfloat16 [32, 64, 4096], P(None, 'dp')
- cur_len: int32 [64], P('dp')
- k_cache: bfloat16 [2, 64, 64, 16, 256], P(None, 'dp', None, 'tp')
- v_cache: bfloat16 [2, 64, 64, 16, 256], P(None, 'dp', None, 'tp')
- ln_gain: bfloat16 [2, 4096], replicated
- ln_bias: bfloat16 [2, 4096], replicated
- w_q: bfloat16 [2, 4096, 4096], P(None, None, 'tp')
- w_k: bfloat16 [2, 4096, 4096], P(None, None, 'tp')
- w_v: bfloat16 [2, 4096, 4096], P(None, None, 'tp')
- w_o: bfloat16 [2, 4096, 4096], P(None, 'tp')
- w_in: bfloat16 [2, 4096, 16384], P(None, None, 'tp')
- b_in: bfloat16 [2, 16384], P(None, 'tp')
- w_out: bfloat16 [2, 16384, 4096], P(None, 'tp')
- b_out: bfloat16 [2, 4096], replicated
Outputs:
- output 1: bfloat16 [32, 64, 4096], P(None, 'dp')
- output 2: bfloat16 [2, 64, 64, 16, 256], P(None, 'dp', None, 'tp')
- output 3: bfloat16 [2, 64, 64, 16, 256], P(None, 'dp', None, 'tp')
All inputs are finite; a program needn't handle non-finite values.
Results may differ from the reference program's by a relative error of at most 0.0162712.
Values are sent between devices in bfloat16 or wider.
A program may use at most 1 GiB of HBM per device.

```python
import jax
import jax.numpy as jnp
from jax import lax

D_MODEL = 4096
N_HEADS = 16
HEAD_DIM = 256
ROT_DIM = 64
FF_DIM = 16384
BATCH_PART = 64
CACHE_LEN = 64
N_STEPS = 32
N_LAYERS = 2
LN_EPS = 1e-5
QUERY_GAIN = 2.5


def setup_inputs(seed: int = 0, part: int = 0) -> dict:
    base_key = jax.random.key(seed)
    shared_keys = jax.random.split(base_key, 10)
    part_keys = jax.random.split(jax.random.fold_in(base_key, part), 6)
    scale_model = D_MODEL ** -0.5
    scale_ff = FF_DIM ** -0.5
    cache_shape = (N_LAYERS, BATCH_PART, CACHE_LEN, N_HEADS, HEAD_DIM)

    def gaussian(key, shape, scale):
        return jax.random.normal(key, shape, jnp.float32) * scale

    top_len = CACHE_LEN - N_STEPS
    raw_span = jax.random.randint(part_keys[1], (BATCH_PART,), 0, top_len)
    shift_bits = jax.random.randint(part_keys[2], (BATCH_PART,), 0, 8)
    full_row = jax.random.randint(part_keys[3], (), 0, BATCH_PART)
    cur_len = 1 + jnp.right_shift(raw_span, shift_bits)
    cur_len = jnp.where(jnp.arange(BATCH_PART) == full_row, top_len, cur_len).astype(jnp.int32)
    return {
        "x_steps": gaussian(part_keys[0], (N_STEPS, BATCH_PART, D_MODEL), 1.0).astype(jnp.bfloat16),
        "cur_len": cur_len,
        "k_cache": gaussian(part_keys[4], cache_shape, 1.0).astype(jnp.bfloat16),
        "v_cache": gaussian(part_keys[5], cache_shape, 1.0).astype(jnp.bfloat16),
        "ln_gain": (1.0 + gaussian(shared_keys[0], (N_LAYERS, D_MODEL), 0.2)).astype(jnp.bfloat16),
        "ln_bias": gaussian(shared_keys[1], (N_LAYERS, D_MODEL), 0.2).astype(jnp.bfloat16),
        "w_q": gaussian(shared_keys[2], (N_LAYERS, D_MODEL, D_MODEL), QUERY_GAIN * scale_model).astype(jnp.bfloat16),
        "w_k": gaussian(shared_keys[3], (N_LAYERS, D_MODEL, D_MODEL), scale_model).astype(jnp.bfloat16),
        "w_v": gaussian(shared_keys[4], (N_LAYERS, D_MODEL, D_MODEL), scale_model).astype(jnp.bfloat16),
        "w_o": gaussian(shared_keys[5], (N_LAYERS, D_MODEL, D_MODEL), scale_model).astype(jnp.bfloat16),
        "w_in": gaussian(shared_keys[6], (N_LAYERS, D_MODEL, FF_DIM), scale_model).astype(jnp.bfloat16),
        "b_in": gaussian(shared_keys[7], (N_LAYERS, FF_DIM), 0.5).astype(jnp.bfloat16),
        "w_out": gaussian(shared_keys[8], (N_LAYERS, FF_DIM, D_MODEL), scale_ff).astype(jnp.bfloat16),
        "b_out": gaussian(shared_keys[9], (N_LAYERS, D_MODEL), 0.3).astype(jnp.bfloat16),
    }


def layer_norm(hidden, gain, bias):
    hid_f32 = hidden.astype(jnp.float32)
    row_mean = jnp.mean(hid_f32, axis=-1, keepdims=True)
    centered = hid_f32 - row_mean
    row_var = jnp.mean(centered * centered, axis=-1, keepdims=True)
    normed = centered / jnp.sqrt(row_var + LN_EPS)
    return (normed * gain.astype(jnp.float32) + bias.astype(jnp.float32)).astype(jnp.bfloat16)


def rotary_tables(positions):
    inv_freq = 1.0 / (10000.0 ** (jnp.arange(0, ROT_DIM, 2).astype(jnp.float32) / ROT_DIM))
    angles = positions.astype(jnp.float32)[:, None] * inv_freq[None, :]
    return jnp.cos(angles)[:, None, :], jnp.sin(angles)[:, None, :]


def apply_rotary(vectors, cos_tab, sin_tab):
    lead_shape = vectors.shape[:-1]
    pairs = vectors[..., :ROT_DIM].reshape(lead_shape + (ROT_DIM // 2, 2))
    even_part = pairs[..., 0]
    odd_part = pairs[..., 1]
    rotated = jnp.stack([even_part * cos_tab - odd_part * sin_tab, odd_part * cos_tab + even_part * sin_tab], axis=-1)
    return jnp.concatenate([rotated.reshape(lead_shape + (ROT_DIM,)), vectors[..., ROT_DIM:]], axis=-1)


def decoder_layer(hidden, new_pos, layer):
    (k_layer, v_layer, gain, bias, q_weight, k_weight, v_weight, o_weight,
     in_weight, in_bias, out_weight, out_bias) = layer
    batch = hidden.shape[0]
    head_shape = (batch, N_HEADS, HEAD_DIM)
    normed = layer_norm(hidden, gain, bias)
    query = jnp.dot(normed, q_weight, preferred_element_type=jnp.float32).reshape(head_shape)
    key_new = jnp.dot(normed, k_weight, preferred_element_type=jnp.float32).reshape(head_shape)
    value_new = jnp.dot(normed, v_weight, preferred_element_type=jnp.float32).reshape(head_shape).astype(jnp.bfloat16)
    cos_tab, sin_tab = rotary_tables(new_pos)
    query = apply_rotary(query, cos_tab, sin_tab).astype(jnp.bfloat16)
    key_new = apply_rotary(key_new, cos_tab, sin_tab).astype(jnp.bfloat16)
    slot_ids = jnp.arange(CACHE_LEN)
    written = (slot_ids[None, :] == new_pos[:, None])[:, :, None, None]
    k_layer = jnp.where(written, key_new[:, None], k_layer)
    v_layer = jnp.where(written, value_new[:, None], v_layer)
    scores = jnp.einsum("bhe,bshe->bhs", query.astype(jnp.float32), k_layer.astype(jnp.float32)) * (HEAD_DIM ** -0.5)
    visible = (slot_ids[None, :] <= new_pos[:, None])[:, None, :]
    scores = jnp.where(visible, scores, -jnp.inf)
    exp_scores = jnp.exp(scores - jnp.max(scores, axis=-1, keepdims=True))
    attn_probs = (exp_scores / jnp.sum(exp_scores, axis=-1, keepdims=True)).astype(jnp.bfloat16)
    context = jnp.einsum("bhs,bshe->bhe", attn_probs.astype(jnp.float32), v_layer.astype(jnp.float32))
    context = context.astype(jnp.bfloat16).reshape(batch, N_HEADS * HEAD_DIM)
    attn_out = jnp.dot(context, o_weight, preferred_element_type=jnp.float32)
    pre_act = jnp.dot(normed, in_weight, preferred_element_type=jnp.float32) + in_bias.astype(jnp.float32)
    gelu_act = jax.nn.gelu(pre_act, approximate=True).astype(jnp.bfloat16)
    mlp_out = jnp.dot(gelu_act, out_weight, preferred_element_type=jnp.float32)
    new_hidden = (hidden.astype(jnp.float32) + attn_out + mlp_out + out_bias.astype(jnp.float32)).astype(jnp.bfloat16)
    return new_hidden, (k_layer, v_layer)


def reference(x_steps, cur_len, k_cache, v_cache, ln_gain, ln_bias, w_q, w_k, w_v, w_o, w_in, b_in, w_out, b_out):
    def one_step(caches, step_in):
        x_now, step_idx = step_in
        new_pos = cur_len + step_idx

        def layer_step(hidden, layer):
            return decoder_layer(hidden, new_pos, layer)

        layers = (caches[0], caches[1], ln_gain, ln_bias, w_q, w_k, w_v, w_o, w_in, b_in, w_out, b_out)
        last_hidden, new_caches = lax.scan(layer_step, x_now, layers)
        return new_caches, last_hidden

    final_caches, hidden_out = lax.scan(one_step, (k_cache, v_cache), (x_steps, jnp.arange(N_STEPS, dtype=jnp.int32)))
    return hidden_out, final_caches[0], final_caches[1]
```

```python
import jax
import jax.numpy as jnp
from jax import lax
from jax.sharding import PartitionSpec as P

ROT_DIM = 64
LN_EPS = 1e-5
N_CHUNKS = 2


def layer_norm(hidden, gain, bias):
    hid_f32 = hidden.astype(jnp.float32)
    row_mean = jnp.mean(hid_f32, axis=-1, keepdims=True)
    centered = hid_f32 - row_mean
    row_var = jnp.mean(centered * centered, axis=-1, keepdims=True)
    normed = centered * lax.rsqrt(row_var + LN_EPS)
    return (normed * gain.astype(jnp.float32) + bias.astype(jnp.float32)).astype(jnp.bfloat16)


def apply_rotary(vec, cos_tab, sin_tab):
    lead = vec.shape[:-1]
    pairs = vec[..., :ROT_DIM].reshape(lead + (ROT_DIM // 2, 2))
    even, odd = pairs[..., 0], pairs[..., 1]
    rot = jnp.stack([even * cos_tab - odd * sin_tab, odd * cos_tab + even * sin_tab], axis=-1)
    return jnp.concatenate([rot.reshape(lead + (ROT_DIM,)), vec[..., ROT_DIM:]], axis=-1)


def layer_part(normed, cur_len, k_old, v_old, weights):
    w_q, w_k, w_v, w_o, w_in, b_in, w_out = weights
    batch, slots, heads, dim = k_old.shape
    steps = normed.shape[0] // batch
    pos = cur_len[None, :] + jnp.arange(steps)[:, None]
    inv_freq = 1.0 / (10000.0 ** (jnp.arange(0, ROT_DIM, 2).astype(jnp.float32) / ROT_DIM))
    angles = pos.astype(jnp.float32)[..., None] * inv_freq
    cos_tab, sin_tab = jnp.cos(angles)[:, :, None, :], jnp.sin(angles)[:, :, None, :]
    shape = (steps, batch, heads, dim)
    query = jnp.dot(normed, w_q, preferred_element_type=jnp.float32).reshape(shape)
    key = jnp.dot(normed, w_k, preferred_element_type=jnp.float32).reshape(shape)
    value = jnp.dot(normed, w_v, preferred_element_type=jnp.float32).astype(jnp.bfloat16).reshape(shape)
    query = apply_rotary(query, cos_tab, sin_tab).astype(jnp.bfloat16)
    key = apply_rotary(key, cos_tab, sin_tab).astype(jnp.bfloat16)
    slot_ids = jnp.arange(slots)
    onehot = (slot_ids[None, :, None] == pos.T[:, None, :]).astype(jnp.bfloat16)
    written = jnp.any(onehot > 0, axis=-1)[:, :, None, None]
    k_all = jnp.where(written, jnp.einsum("bst,tbhe->bshe", onehot, key), k_old)
    v_all = jnp.where(written, jnp.einsum("bst,tbhe->bshe", onehot, value), v_old)
    scores = jnp.einsum("tbhe,bshe->bhts", query, k_all, preferred_element_type=jnp.float32) * (dim ** -0.5)
    visible = slot_ids[None, None, :] <= pos.T[:, :, None]
    scores = jnp.where(visible[:, None], scores, -jnp.inf)
    exps = jnp.exp(scores - jnp.max(scores, axis=-1, keepdims=True))
    probs = (exps / jnp.sum(exps, axis=-1, keepdims=True)).astype(jnp.bfloat16)
    context = jnp.einsum("bhts,bshe->tbhe", probs, v_all, preferred_element_type=jnp.float32).astype(jnp.bfloat16)
    context = context.reshape(steps * batch, heads * dim)
    pre_act = jnp.dot(normed, w_in, preferred_element_type=jnp.float32) + b_in.astype(jnp.float32)
    act = jax.nn.gelu(pre_act, approximate=True).astype(jnp.bfloat16)
    part = jnp.dot(context, w_o, preferred_element_type=jnp.float32) + jnp.dot(act, w_out, preferred_element_type=jnp.float32)
    return part.astype(jnp.bfloat16), k_all, v_all


def decode_shard(x_steps, cur_len, k_cache, v_cache, ln_gain, ln_bias, w_q, w_k, w_v, w_o, w_in, b_in, w_out, b_out):
    n_layers = k_cache.shape[0]
    steps, batch, width = x_steps.shape
    n_dev = lax.axis_size("tp")
    me = lax.axis_index("tp")
    group = batch // N_CHUNKS
    hiddens, normeds, outs = [], [], []
    k_new = [[None] * N_CHUNKS for _ in range(n_layers)]
    v_new = [[None] * N_CHUNKS for _ in range(n_layers)]
    own_rows = steps * group // n_dev
    for c in range(N_CHUNKS):
        rows = x_steps[:, c * group:(c + 1) * group].reshape(steps * group, width)
        hiddens.append(lax.dynamic_slice_in_dim(rows, me * own_rows, own_rows, 0))
        normeds.append(layer_norm(rows, ln_gain[0], ln_bias[0]))
    for layer in range(n_layers):
        weights = (w_q[layer], w_k[layer], w_v[layer], w_o[layer], w_in[layer], b_in[layer], w_out[layer])
        for c in range(N_CHUNKS):
            seqs = slice(c * group, (c + 1) * group)
            part, k_new[layer][c], v_new[layer][c] = layer_part(normeds[c], cur_len[seqs], k_cache[layer, seqs], v_cache[layer, seqs], weights)
            total = lax.psum_scatter(part, "tp", scatter_dimension=0, tiled=True)
            hiddens[c] = (hiddens[c].astype(jnp.float32) + total.astype(jnp.float32) + b_out[layer].astype(jnp.float32)).astype(jnp.bfloat16)
            if layer + 1 < n_layers:
                send = layer_norm(hiddens[c], ln_gain[layer + 1], ln_bias[layer + 1])
            else:
                send = hiddens[c]
            normeds[c] = lax.all_gather(send, "tp", axis=0, tiled=True)
    hidden_out = jnp.concatenate([n.reshape(steps, group, width) for n in normeds], axis=1)
    k_out = jnp.stack([jnp.concatenate(ks, axis=0) for ks in k_new])
    v_out = jnp.stack([jnp.concatenate(vs, axis=0) for vs in v_new])
    return hidden_out, k_out, v_out


def solution(mesh):
    cache_spec = P(None, "dp", None, "tp", None)
    in_specs = (P(None, "dp", None), P("dp"), cache_spec, cache_spec, P(None, None), P(None, None),
                P(None, None, "tp"), P(None, None, "tp"), P(None, None, "tp"), P(None, "tp", None),
                P(None, None, "tp"), P(None, "tp"), P(None, "tp", None), P(None, None))
    out_specs = (P(None, "dp", None), cache_spec, cache_spec)
    return jax.shard_map(decode_shard, mesh=mesh, in_specs=in_specs, out_specs=out_specs, check_vma=False)
```

```python
import functools

import jax
import jax.numpy as jnp
from jax import lax
from jax.experimental import pallas as pl
from jax.experimental.pallas import tpu as pltpu
from jax.sharding import PartitionSpec as P

MESH = pl.DeviceIdType.MESH
ROT_DIM = 64
LN_EPS = 1e-5
GELU_C = 0.7978845608028654
WIDTH, HEAD, STEPS, SLOTS, HEADS = 4096, 256, 32, 64, 2
GROUP = 16
N_GROUPS, N_LAYERS = 4, 2
N_TASKS = N_GROUPS * N_LAYERS
ROWS = STEPS * GROUP
FF, ATT = 2048, 512
TILE = 256
T_QKV, T_IN, T_OUT = 3 * ATT // TILE, FF // TILE, WIDTH // TILE
T_ALL = T_QKV + T_IN + T_OUT
NBUF = 4
RS0, RS1, RS2, AGA, AGB, AGC = range(6)


def norm_rows(x, gain, bias):
    mean = jnp.mean(x, axis=-1, keepdims=True)
    centered = x - mean
    var = jnp.mean(centered * centered, axis=-1, keepdims=True)
    return (centered * lax.rsqrt(var + LN_EPS) * gain + bias).astype(jnp.bfloat16)


def kernel(cur_ref, x_hbm, kc_hbm, vc_hbm, gain_ref, bias_ref, bout_ref, bin_ref, cos_ref, sin_ref,
           wq, wk, wv, wo, win, wout, out_hbm, ko_hbm, vo_hbm,
           hbuf, gbuf, pbuf, r0, r1, r2, xres, qkv, ctx, act, wbuf, kbuf, vbuf,
           wsem, hsem, csem, cosem, xsem, gsem, ssem, rsem, ready, r0free):
    me = lax.axis_index("tp")
    core = me % 2
    xc = (me // 2) % 2
    yc = me // 4
    sib = me + 1 - 2 * core
    xn = me + 2 - 4 * xc
    yn = me + 4 - 8 * yc
    a1 = (1 - core) * xc + core * yc
    a2 = (1 - core) * yc + core * xc
    p1 = (1 - core) * xn + core * yn
    p2 = (1 - core) * yn + core * xn
    half = 16 * core
    quarter = half + 8 * a1
    own = quarter + 4 * a2
    partners = (sib, p1, p2)

    barrier = pltpu.get_barrier_semaphore()
    for dev in partners:
        pl.semaphore_signal(barrier, inc=1, device_id={"tp": dev}, device_id_type=MESH)
    pl.semaphore_wait(barrier, 3)

    def remote(src, dst, idx, dev):
        return pltpu.make_async_remote_copy(src_ref=src, dst_ref=dst, send_sem=ssem.at[idx], recv_sem=rsem.at[idx],
                                            device_id={"tp": dev}, device_id_type=MESH)

    def issue(u):
        @pl.when(u < N_TASKS * T_ALL)
        def _():
            task, j = u // T_ALL, u % T_ALL
            layer = task // N_GROUPS
            b = u % NBUF
            for k, ref in enumerate((wq, wk, wv)):
                @pl.when((j >= 2 * k) & (j < 2 * k + 2))
                def _():
                    col = pl.multiple_of((j - 2 * k) * TILE, TILE)
                    pltpu.make_async_copy(ref.at[layer, :, pl.ds(col, TILE)], wbuf.at[b], wsem.at[b]).start()

            @pl.when((j >= T_QKV) & (j < T_QKV + T_IN))
            def _():
                col = pl.multiple_of((j - T_QKV) * TILE, TILE)
                pltpu.make_async_copy(win.at[layer, :, pl.ds(col, TILE)], wbuf.at[b], wsem.at[b]).start()

            @pl.when(j >= T_QKV + T_IN)
            def _():
                col = pl.multiple_of((j - T_QKV - T_IN) * TILE, TILE)
                pltpu.make_async_copy(wo.at[layer, :, pl.ds(col, TILE)], wbuf.at[b, pl.ds(0, ATT), :], wsem.at[b]).start()
                pltpu.make_async_copy(wout.at[layer, :, pl.ds(col, TILE)], wbuf.at[b, pl.ds(ATT, FF), :], wsem.at[b]).start()

    def load_h(task):
        c = task % N_GROUPS
        b = task % 2
        cols = pl.ds(pl.multiple_of(c * GROUP, GROUP), GROUP)

        @pl.when(task < N_GROUPS)
        def _():
            pltpu.make_async_copy(x_hbm.at[:, cols, :], hbuf.at[b], hsem.at[b]).start()

        @pl.when((task >= N_GROUPS) & (task < N_TASKS))
        def _():
            pltpu.make_async_copy(out_hbm.at[:, cols, :], hbuf.at[b], hsem.at[b]).start()

    def add_rows(p, base, r_ref, rbase, n):
        def body(t, _):
            pbuf[p, base + t] = (pbuf[p, base + t].astype(jnp.float32) + r_ref[rbase + t].astype(jnp.float32)).astype(jnp.bfloat16)
            return 0
        lax.fori_loop(0, n, body, 0)

    for u in range(NBUF):
        issue(u)
    load_h(0)

    row_i = lax.broadcasted_iota(jnp.int32, (2 * SLOTS, 2 * STEPS), 0)
    col_i = lax.broadcasted_iota(jnp.int32, (2 * SLOTS, 2 * STEPS), 1)
    put_same = (row_i % 2) == (col_i // STEPS)
    put_off = row_i // 2 - col_i % STEPS
    wr_slot = lax.broadcasted_iota(jnp.int32, (2 * SLOTS, HEAD), 0) // 2
    s_row = lax.broadcasted_iota(jnp.int32, (2 * STEPS, 2 * SLOTS), 0)
    s_col = lax.broadcasted_iota(jnp.int32, (2 * STEPS, 2 * SLOTS), 1)
    see_same = (s_row // STEPS) == (s_col % 2)
    see_off = s_col // 2 - s_row % STEPS
    even_lane = lax.broadcasted_iota(jnp.int32, (STEPS, 128), 1) % 2 == 0

    def slot(s, _):
        pn, po = s % 2, (s + 1) % 2
        gb, gn = s % 2, (s + 1) % 2
        hb = s % 2
        layer, c = s // N_GROUPS, s % N_GROUPS
        l1, c1 = (s + N_GROUPS - 1) // N_GROUPS - 1, (s + N_GROUPS - 1) % N_GROUPS
        c2 = (s + N_GROUPS - 2) % N_GROUPS
        do_c = s < N_TASKS
        do_rs = (s >= 1) & (s <= N_TASKS)
        do_ag = s >= 2
        cseq = pl.multiple_of(c * GROUP, GROUP)

        def mm1_tile(j):
            u = s * T_ALL + j
            b = u % NBUF
            pltpu.make_async_copy(win.at[0, :, pl.ds(0, TILE)], wbuf.at[b], wsem.at[b]).wait()
            acc = jnp.dot(hbuf[hb].reshape(ROWS, WIDTH), wbuf[b], preferred_element_type=jnp.float32)
            return acc, u

        @pl.when(do_rs)
        def _():
            remote(pbuf.at[po, pl.ds(16 - half, 16)], r0, RS0, sib).wait()
            add_rows(po, half + 8 * (1 - a1), r0, 8 * (1 - a1), 8)

        @pl.when(s >= 1)
        def _():
            pl.semaphore_wait(ready.at[1], 1)
            pl.semaphore_wait(ready.at[2], 1)

        @pl.when(do_ag)
        def _():
            remote(gbuf.at[gb, pl.ds(own, 4)], gbuf.at[gb, pl.ds(own, 4)], AGA, p2).start()

        @pl.when(do_rs)
        def _():
            remote(pbuf.at[po, pl.ds(half + 8 * (1 - a1), 8)], r1, RS1, p1).start()
            add_rows(po, quarter, r0, 8 * a1, 8)

        @pl.when((s >= 1) & (s < N_TASKS))
        def _():
            pl.semaphore_signal(r0free, inc=1, device_id={"tp": sib}, device_id_type=MESH)

        @pl.when(do_c)
        def _():
            @pl.when(s >= 1)
            def _():
                pltpu.make_async_copy(kbuf, ko_hbm.at[0, pl.ds(0, GROUP)], cosem.at[0]).wait()
                pltpu.make_async_copy(vbuf, vo_hbm.at[0, pl.ds(0, GROUP)], cosem.at[1]).wait()
            pltpu.make_async_copy(kc_hbm.at[layer, pl.ds(cseq, GROUP)], kbuf, csem.at[0]).start()
            pltpu.make_async_copy(vc_hbm.at[layer, pl.ds(cseq, GROUP)], vbuf, csem.at[1]).start()
            pltpu.make_async_copy(x_hbm.at[:, pl.ds(0, GROUP), :], hbuf.at[hb], hsem.at[hb]).wait()

            @pl.when(layer == 0)
            def _():
                def ln(t, _):
                    hbuf[hb, t] = norm_rows(hbuf[hb, t].astype(jnp.float32), gain_ref[0], bias_ref[0])
                    return 0
                lax.fori_loop(0, STEPS, ln, 0)

            def qkv_tile(j, _):
                acc, u = mm1_tile(j)
                qkv[2 * j] = acc[:, :128]
                qkv[2 * j + 1] = acc[:, 128:]
                issue(u + NBUF)
                return 0
            lax.fori_loop(0, T_QKV, qkv_tile, 0)

        @pl.when(do_ag)
        def _():
            remote(gbuf.at[gb, pl.ds(own, 4)], gbuf.at[gb, pl.ds(own, 4)], AGA, p2).wait()
            remote(gbuf.at[gb, pl.ds(quarter, 8)], gbuf.at[gb, pl.ds(quarter, 8)], AGB, p1).start()

        @pl.when(s >= 3)
        def _():
            pltpu.make_async_copy(gbuf.at[gn], out_hbm.at[:, pl.ds(0, GROUP), :], gsem).wait()

        load_h(s + 1)

        @pl.when(do_rs & (l1 == 0))
        def _():
            pltpu.make_async_copy(x_hbm.at[pl.ds(own, 4), pl.ds(pl.multiple_of(c1 * GROUP, GROUP), GROUP), :], xres.at[c1], xsem).start()

        def in_tile(j, _):
            acc, u = mm1_tile(T_QKV + j)
            y = acc + bin_ref[layer, j]
            g = 0.5 * y * (1.0 + jnp.tanh(GELU_C * (y + 0.044715 * y * y * y)))
            act[:, pl.ds(pl.multiple_of(ATT + j * TILE, TILE), TILE)] = g.astype(jnp.bfloat16)
            issue(u + NBUF)
            return 0

        @pl.when(do_c)
        def _():
            lax.fori_loop(0, T_IN // 2, in_tile, 0)

        @pl.when(do_rs)
        def _():
            remote(pbuf.at[po, pl.ds(half + 8 * (1 - a1), 8)], r1, RS1, p1).wait()
            add_rows(po, quarter + 4 * (1 - a2), r1, 4 * (1 - a2), 4)
            remote(pbuf.at[po, pl.ds(quarter + 4 * (1 - a2), 4)], r2, RS2, p2).start()
            add_rows(po, own, r1, 4 * a2, 4)

        def attend(i, _):
            b = c * GROUP + i
            cur = cur_ref[b]
            cos_t, sin_t = cos_ref[b], sin_ref[b]

            def part(k, rotary):
                lo = qkv[2 * k, pl.ds(i, STEPS, stride=GROUP), :]
                hi = qkv[2 * k + 1, pl.ds(i, STEPS, stride=GROUP), :]
                if rotary:
                    other = jnp.where(even_lane, pltpu.roll(lo, 127, 1), pltpu.roll(lo, 1, 1))
                    lo = lo * cos_t + other * sin_t
                return jnp.concatenate([lo, hi], axis=1)

            q = jnp.concatenate([part(0, True), part(1, True)], axis=0).astype(jnp.bfloat16)
            k_new = jnp.concatenate([part(2, True), part(3, True)], axis=0).astype(jnp.bfloat16)
            v_new = jnp.concatenate([part(4, False), part(5, False)], axis=0).astype(jnp.bfloat16)
            put = jnp.where(put_same & (put_off == cur), 1.0, 0.0).astype(jnp.bfloat16)
            written = (wr_slot >= cur) & (wr_slot < cur + STEPS)
            k_all = jnp.where(written, jnp.dot(put, k_new, preferred_element_type=jnp.float32), kbuf[i].astype(jnp.float32)).astype(jnp.bfloat16)
            v_all = jnp.where(written, jnp.dot(put, v_new, preferred_element_type=jnp.float32), vbuf[i].astype(jnp.float32)).astype(jnp.bfloat16)
            kbuf[i] = k_all
            vbuf[i] = v_all
            sc = lax.dot_general(q, k_all, (((1,), (1,)), ((), ())), preferred_element_type=jnp.float32) * (HEAD ** -0.5)
            sc = jnp.where(see_same & (see_off <= cur), sc, -jnp.inf)
            ex = jnp.exp(sc - jnp.max(sc, axis=-1, keepdims=True))
            pr = (ex / jnp.sum(ex, axis=-1, keepdims=True)).astype(jnp.bfloat16)
            cx = jnp.dot(pr, v_all, preferred_element_type=jnp.float32)
            for h in range(HEADS):
                for w in range(2):
                    ctx[2 * h + w, pl.ds(i, STEPS, stride=GROUP), :] = cx[h * STEPS:(h + 1) * STEPS, w * 128:(w + 1) * 128]
            return 0

        def out_tile(j, _):
            u = s * T_ALL + T_QKV + T_IN + j
            b = u % NBUF
            pltpu.make_async_copy(win.at[0, pl.ds(0, ATT + FF), pl.ds(0, TILE)], wbuf.at[b, pl.ds(0, ATT + FF), :], wsem.at[b]).wait()
            acc = jnp.dot(act[...], wbuf[b, :ATT + FF, :], preferred_element_type=jnp.float32)
            pbuf[pn, :, :, pl.ds(pl.multiple_of(j * TILE, TILE), TILE)] = acc.astype(jnp.bfloat16).reshape(STEPS, GROUP, TILE)

            @pl.when(j >= 1)
            def _():
                send_half(j - 1)
            issue(u + NBUF)
            return 0

        def send_half(j):
            cols = pl.ds(pl.multiple_of(j * TILE, TILE), TILE)
            remote(pbuf.at[pn, pl.ds(16 - half, 16), :, cols], r0.at[:, :, cols], RS0, sib).start()

        @pl.when(do_c)
        def _():
            lax.fori_loop(T_IN // 2, T_IN, in_tile, 0)
            pltpu.make_async_copy(kc_hbm.at[0, pl.ds(0, GROUP)], kbuf, csem.at[0]).wait()
            pltpu.make_async_copy(vc_hbm.at[0, pl.ds(0, GROUP)], vbuf, csem.at[1]).wait()
            lax.fori_loop(0, GROUP, attend, 0)
            pltpu.make_async_copy(kbuf, ko_hbm.at[layer, pl.ds(cseq, GROUP)], cosem.at[0]).start()
            pltpu.make_async_copy(vbuf, vo_hbm.at[layer, pl.ds(cseq, GROUP)], cosem.at[1]).start()
            for k in range(4):
                act[:, k * 128:(k + 1) * 128] = ctx[k].astype(jnp.bfloat16)

            @pl.when(s >= 1)
            def _():
                pl.semaphore_wait(r0free, 1)
            lax.fori_loop(0, T_OUT // 2, out_tile, 0)

        @pl.when(do_rs)
        def _():
            remote(pbuf.at[po, pl.ds(quarter + 4 * (1 - a2), 4)], r2, RS2, p2).wait()

            @pl.when(l1 == 0)
            def _():
                pltpu.make_async_copy(x_hbm.at[pl.ds(0, 4), pl.ds(0, GROUP), :], xres.at[c1], xsem).wait()

            def finish(t, _):
                tot = pbuf[po, own + t].astype(jnp.float32) + r2[t].astype(jnp.float32)
                new = (xres[c1, t].astype(jnp.float32) + tot + bout_ref[l1]).astype(jnp.bfloat16)

                @pl.when(l1 == 0)
                def _():
                    xres[c1, t] = new
                    gbuf[gn, own + t] = norm_rows(new.astype(jnp.float32), gain_ref[1], bias_ref[1])

                @pl.when(l1 == 1)
                def _():
                    gbuf[gn, own + t] = new
                return 0
            lax.fori_loop(0, 4, finish, 0)

        @pl.when(do_ag)
        def _():
            remote(gbuf.at[gb, pl.ds(quarter, 8)], gbuf.at[gb, pl.ds(quarter, 8)], AGB, p1).wait()

        @pl.when(s <= N_TASKS)
        def _():
            for k in (1, 2):
                pl.semaphore_signal(ready.at[k], inc=1, device_id={"tp": partners[k]}, device_id_type=MESH)

        @pl.when(s >= 1)
        def _():
            pl.semaphore_wait(ready.at[0], 1)

        @pl.when(do_ag)
        def _():
            remote(gbuf.at[gb, pl.ds(half, 16)], gbuf.at[gb, pl.ds(half, 16)], AGC, sib).start()

        @pl.when(do_c)
        def _():
            lax.fori_loop(T_OUT // 2, T_OUT, out_tile, 0)
            send_half(T_OUT - 1)

        @pl.when(do_ag)
        def _():
            remote(gbuf.at[gb, pl.ds(half, 16)], gbuf.at[gb, pl.ds(half, 16)], AGC, sib).wait()
            pltpu.make_async_copy(gbuf.at[gb], out_hbm.at[:, pl.ds(pl.multiple_of(c2 * GROUP, GROUP), GROUP), :], gsem).start()

        @pl.when(s <= N_TASKS)
        def _():
            pl.semaphore_signal(ready.at[0], inc=1, device_id={"tp": sib}, device_id_type=MESH)
        return 0

    lax.fori_loop(0, N_TASKS + 2, slot, 0)
    pltpu.make_async_copy(gbuf.at[0], out_hbm.at[:, pl.ds(0, GROUP), :], gsem).wait()
    pltpu.make_async_copy(kbuf, ko_hbm.at[0, pl.ds(0, GROUP)], cosem.at[0]).wait()
    pltpu.make_async_copy(vbuf, vo_hbm.at[0, pl.ds(0, GROUP)], cosem.at[1]).wait()


def decode_shard(x_steps, cur_len, k_cache, v_cache, ln_gain, ln_bias, w_q, w_k, w_v, w_o, w_in, b_in, w_out, b_out):
    n_layers, batch, slots, heads, dim = k_cache.shape
    f32 = jnp.float32
    lane = jnp.arange(128)
    inv_freq = jnp.where(lane < ROT_DIM, 1.0 / (10000.0 ** ((lane // 2 * 2).astype(f32) / ROT_DIM)), 0.0)
    pos = (cur_len[:, None] + jnp.arange(STEPS)[None, :]).astype(f32)
    angles = pos[:, :, None] * inv_freq
    cos_tab = jnp.cos(angles)
    sin_tab = jnp.sin(angles) * jnp.where(lane % 2 == 0, -1.0, 1.0)
    flat = (n_layers, batch, slots * heads, dim)
    bf = jnp.bfloat16
    any_spec, vmem = pl.BlockSpec(memory_space=pl.ANY), pl.BlockSpec(memory_space=pltpu.VMEM)
    out, k_out, v_out = pl.pallas_call(
        kernel,
        out_shape=(jax.ShapeDtypeStruct(x_steps.shape, bf), jax.ShapeDtypeStruct(flat, bf), jax.ShapeDtypeStruct(flat, bf)),
        in_specs=[pl.BlockSpec(memory_space=pltpu.SMEM), any_spec, any_spec, any_spec] + [vmem] * 6 + [any_spec] * 6,
        out_specs=(any_spec, any_spec, any_spec),
        scratch_shapes=[
            pltpu.VMEM((2, STEPS, GROUP, WIDTH), bf),
            pltpu.VMEM((2, STEPS, GROUP, WIDTH), bf),
            pltpu.VMEM((2, STEPS, GROUP, WIDTH), bf),
            pltpu.VMEM((16, GROUP, WIDTH), bf),
            pltpu.VMEM((8, GROUP, WIDTH), bf),
            pltpu.VMEM((4, GROUP, WIDTH), bf),
            pltpu.VMEM((N_GROUPS, 4, GROUP, WIDTH), bf),
            pltpu.VMEM((12, ROWS, 128), f32),
            pltpu.VMEM((4, ROWS, 128), f32),
            pltpu.VMEM((ROWS, ATT + FF), bf),
            pltpu.VMEM((NBUF, WIDTH, TILE), bf),
            pltpu.VMEM((GROUP, 2 * SLOTS, HEAD), bf),
            pltpu.VMEM((GROUP, 2 * SLOTS, HEAD), bf),
            pltpu.SemaphoreType.DMA((NBUF,)),
            pltpu.SemaphoreType.DMA((2,)),
            pltpu.SemaphoreType.DMA((2,)),
            pltpu.SemaphoreType.DMA((2,)),
            pltpu.SemaphoreType.DMA,
            pltpu.SemaphoreType.DMA,
            pltpu.SemaphoreType.DMA((6,)),
            pltpu.SemaphoreType.DMA((6,)),
            pltpu.SemaphoreType.REGULAR((3,)),
            pltpu.SemaphoreType.REGULAR,
        ],
        compiler_params=pltpu.CompilerParams(collective_id=0, has_side_effects=True, vmem_limit_bytes=62 * 1024 * 1024),
    )(cur_len, x_steps, k_cache.reshape(flat), v_cache.reshape(flat),
      ln_gain.astype(f32)[:, None], ln_bias.astype(f32)[:, None], b_out.astype(f32)[:, None],
      b_in.astype(f32).reshape(n_layers, T_IN, 1, TILE), cos_tab, sin_tab, w_q, w_k, w_v, w_o, w_in, w_out)
    return out, k_out.reshape(k_cache.shape), v_out.reshape(v_cache.shape)


def solution(mesh):
    cache_spec = P(None, "dp", None, "tp", None)
    in_specs = (P(None, "dp", None), P("dp"), cache_spec, cache_spec, P(None, None), P(None, None),
                P(None, None, "tp"), P(None, None, "tp"), P(None, None, "tp"), P(None, "tp", None),
                P(None, None, "tp"), P(None, "tp"), P(None, "tp", None), P(None, None))
    out_specs = (P(None, "dp", None), cache_spec, cache_spec)
    return jax.shard_map(decode_shard, mesh=mesh, in_specs=in_specs, out_specs=out_specs, check_vma=False)
```

```python
import functools

import jax
import jax.numpy as jnp
import numpy as np
from jax import lax
from jax.experimental import pallas as pl
from jax.experimental.pallas import tpu as pltpu
from jax.sharding import PartitionSpec as P

MESH = pl.DeviceIdType.MESH
ROT_DIM = 64
LN_EPS = 1e-5
GELU_C = 0.7978845608028654
WIDTH, HEAD, STEPS, SLOTS, HEADS = 4096, 256, 32, 64, 2
GROUP = 16
N_GROUPS, N_LAYERS = 4, 2
N_TASKS = N_GROUPS * N_LAYERS
ROWS = STEPS * GROUP
FF, ATT = 2048, 512
TILE = 512
T_QKV, T_IN, T_OUT = 3 * ATT // TILE, FF // TILE, WIDTH // TILE
T_ALL = T_QKV + T_IN + T_OUT
NBUF = 3
LN_STEP = 4
AT_STEP = 4
TOP_TILES, OUT_SPLIT = 1, 6
RS0, RS1, RS2, AGA, AGB, AGC = range(6)


def norm_rows(x, gain, bias):
    mean = jnp.mean(x, axis=-1, keepdims=True)
    centered = x - mean
    var = jnp.mean(centered * centered, axis=-1, keepdims=True)
    return (centered * lax.rsqrt(var + LN_EPS) * gain + bias).astype(jnp.bfloat16)


def kernel(cur_ref, x_hbm, kc_hbm, vc_hbm, gain_in, bias_in, bout_in, bin_in, cos_ref, sin_ref,
           wq, wk, wv, wo, win, wout, out_hbm, ko_hbm, vo_hbm,
           hbuf, gbuf, pbuf, r0, r1, r2, xres, qkv, ctx, act, wbuf, kbuf, vbuf, gain_ref, bias_ref, bout_ref, bin_ref,
           wsem, hsem, csem, cosem, xsem, gsem, ssem, rsem, ready, r0free, gfree):
    me = lax.axis_index("tp")
    core = me % 2
    xc = (me // 2) % 2
    yc = me // 4
    sib = me + 1 - 2 * core
    xn = me + 2 - 4 * xc
    yn = me + 4 - 8 * yc
    a1 = (1 - core) * xc + core * yc
    a2 = (1 - core) * yc + core * xc
    p1 = (1 - core) * xn + core * yn
    p2 = (1 - core) * yn + core * xn
    half = 16 * core
    quarter = half + 8 * a1
    own = quarter + 4 * a2
    partners = (sib, p1, p2)

    barrier = pltpu.get_barrier_semaphore()
    for dev in partners:
        pl.semaphore_signal(barrier, inc=1, device_id={"tp": dev}, device_id_type=MESH)
    pl.semaphore_wait(barrier, 3)

    def remote(src, dst, idx, dev):
        return pltpu.make_async_remote_copy(src_ref=src, dst_ref=dst, send_sem=ssem.at[idx], recv_sem=rsem.at[idx],
                                            device_id={"tp": dev}, device_id_type=MESH)

    def issue(u):
        @pl.when(u < N_TASKS * T_ALL)
        def _():
            task, j = u // T_ALL, u % T_ALL
            layer = task // N_GROUPS
            b = u % NBUF
            for k, ref in enumerate((wq, wk, wv)):
                n = ATT // TILE

                @pl.when((j >= n * k) & (j < n * k + n))
                def _():
                    col = pl.multiple_of((j - n * k) * TILE, TILE)
                    pltpu.make_async_copy(ref.at[layer, :, pl.ds(col, TILE)], wbuf.at[b], wsem.at[b]).start()

            @pl.when((j >= T_QKV) & (j < T_QKV + T_IN))
            def _():
                col = pl.multiple_of((j - T_QKV) * TILE, TILE)
                pltpu.make_async_copy(win.at[layer, :, pl.ds(col, TILE)], wbuf.at[b], wsem.at[b]).start()

            @pl.when(j >= T_QKV + T_IN)
            def _():
                col = pl.multiple_of((j - T_QKV - T_IN) * TILE, TILE)
                pltpu.make_async_copy(wo.at[layer, :, pl.ds(col, TILE)], wbuf.at[b, pl.ds(0, ATT), :], wsem.at[b]).start()
                pltpu.make_async_copy(wout.at[layer, :, pl.ds(col, TILE)], wbuf.at[b, pl.ds(ATT, FF), :], wsem.at[b]).start()

    def load_h(task):
        c = task % N_GROUPS
        b = task % 2
        cols = pl.ds(pl.multiple_of(c * GROUP, GROUP), GROUP)

        @pl.when(task < N_GROUPS)
        def _():
            pltpu.make_async_copy(x_hbm.at[:, cols, :], hbuf.at[b], hsem.at[b]).start()

        @pl.when((task >= N_GROUPS) & (task < N_TASKS))
        def _():
            pltpu.make_async_copy(out_hbm.at[:, cols, :], hbuf.at[b], hsem.at[b]).start()

    def add_rows(p, base, r_ref, rbase, n):
        def body(t, _):
            pbuf[p, base + t] = (pbuf[p, base + t].astype(jnp.float32) + r_ref[rbase + t].astype(jnp.float32)).astype(jnp.bfloat16)
            return 0
        lax.fori_loop(0, n, body, 0)

    for u in range(NBUF):
        issue(u)
    load_h(0)
    for l in range(N_LAYERS):
        for dst, src in ((gain_ref, gain_in), (bias_ref, bias_in), (bout_ref, bout_in)):
            dst[l] = src[l:l + 1, :].astype(jnp.float32)
        for j in range(T_IN):
            bin_ref[l, j] = bin_in[l:l + 1, j * TILE:(j + 1) * TILE].astype(jnp.float32)

    row_i = lax.broadcasted_iota(jnp.int32, (2 * SLOTS, 2 * STEPS), 0)
    col_i = lax.broadcasted_iota(jnp.int32, (2 * SLOTS, 2 * STEPS), 1)
    put_same = (row_i % 2) == (col_i // STEPS)
    put_off = row_i // 2 - col_i % STEPS
    wr_slot = lax.broadcasted_iota(jnp.int32, (2 * SLOTS, HEAD), 0) // 2
    s_row = lax.broadcasted_iota(jnp.int32, (2 * STEPS, 2 * SLOTS), 0)
    s_col = lax.broadcasted_iota(jnp.int32, (2 * STEPS, 2 * SLOTS), 1)
    see_same = (s_row // STEPS) == (s_col % 2)
    see_off = s_col // 2 - s_row % STEPS
    even_lane = lax.broadcasted_iota(jnp.int32, (STEPS, 128), 1) % 2 == 0

    def slot(s, _):
        pn, po = s % 2, (s + 1) % 2
        gb, gn = s % 2, (s + 1) % 2
        hb = s % 2
        layer, c = s // N_GROUPS, s % N_GROUPS
        l1, c1 = (s + N_GROUPS - 1) // N_GROUPS - 1, (s + N_GROUPS - 1) % N_GROUPS
        c2 = (s + N_GROUPS - 2) % N_GROUPS
        do_c = s < N_TASKS
        do_rs = (s >= 1) & (s <= N_TASKS)
        do_ag = s >= 2
        cseq = pl.multiple_of(c * GROUP, GROUP)

        def mm1_tile(j):
            u = s * T_ALL + j
            b = u % NBUF
            pltpu.make_async_copy(win.at[0, :, pl.ds(0, TILE)], wbuf.at[b], wsem.at[b]).wait()
            acc = jnp.dot(hbuf[hb].reshape(ROWS, WIDTH), wbuf[b], preferred_element_type=jnp.float32)
            return acc, u

        def qkv_tile(j, _):
            acc, u = mm1_tile(j)
            for w in range(TILE // 128):
                qkv[TILE // 128 * j + w] = acc[:, w * 128:(w + 1) * 128]
            issue(u + NBUF)
            return 0

        @pl.when(do_c)
        def _():
            @pl.when(s >= 1)
            def _():
                pltpu.make_async_copy(kbuf, ko_hbm.at[0, pl.ds(0, GROUP)], cosem.at[0]).wait()
                pltpu.make_async_copy(vbuf, vo_hbm.at[0, pl.ds(0, GROUP)], cosem.at[1]).wait()
            pltpu.make_async_copy(kc_hbm.at[layer, pl.ds(cseq, GROUP)], kbuf, csem.at[0]).start()
            pltpu.make_async_copy(vc_hbm.at[layer, pl.ds(cseq, GROUP)], vbuf, csem.at[1]).start()
            pltpu.make_async_copy(x_hbm.at[:, pl.ds(0, GROUP), :], hbuf.at[hb], hsem.at[hb]).wait()

            @pl.when(layer == 0)
            def _():
                def ln(t, _):
                    done = [norm_rows(hbuf[hb, LN_STEP * t + k].astype(jnp.float32), gain_ref[0], bias_ref[0]) for k in range(LN_STEP)]
                    for k in range(LN_STEP):
                        hbuf[hb, LN_STEP * t + k] = done[k]
                    return 0
                lax.fori_loop(0, STEPS // LN_STEP, ln, 0)

            lax.fori_loop(0, TOP_TILES, qkv_tile, 0)

        @pl.when(do_rs)
        def _():
            remote(pbuf.at[po, pl.ds(16 - half, 16)], r0, RS0, sib).wait()
            add_rows(po, half + 8 * (1 - a1), r0, 8 * (1 - a1), 8)

        @pl.when(s >= 1)
        def _():
            pl.semaphore_wait(ready.at[1], 1)

        @pl.when(do_rs)
        def _():
            remote(pbuf.at[po, pl.ds(half + 8 * (1 - a1), 8)], r1, RS1, p1).start()

        @pl.when(do_ag)
        def _():
            remote(gbuf.at[gb, pl.ds(own, 4)], gbuf.at[gb, pl.ds(own, 4)], AGA, p2).wait()
            remote(gbuf.at[gb, pl.ds(quarter, 8)], gbuf.at[gb, pl.ds(quarter, 8)], AGB, p1).start()

        @pl.when(do_rs)
        def _():
            add_rows(po, quarter, r0, 8 * a1, 8)

        @pl.when((s >= 1) & (s < N_TASKS))
        def _():
            pl.semaphore_signal(r0free, inc=1, device_id={"tp": sib}, device_id_type=MESH)

        @pl.when(do_c)
        def _():
            lax.fori_loop(TOP_TILES, T_QKV, qkv_tile, 0)

        @pl.when(s >= 3)
        def _():
            pltpu.make_async_copy(gbuf.at[gn], out_hbm.at[:, pl.ds(0, GROUP), :], gsem).wait()

        @pl.when(do_rs)
        def _():
            pl.semaphore_signal(gfree, inc=1, device_id={"tp": p2}, device_id_type=MESH)

        load_h(s + 1)

        @pl.when(do_rs & (l1 == 0))
        def _():
            pltpu.make_async_copy(x_hbm.at[pl.ds(own, 4), pl.ds(pl.multiple_of(c1 * GROUP, GROUP), GROUP), :], xres.at[c1], xsem).start()

        def in_tile(j, _):
            acc, u = mm1_tile(T_QKV + j)
            y = acc + bin_ref[layer, j]
            g = 0.5 * y * (1.0 + jnp.tanh(GELU_C * (y + 0.044715 * y * y * y)))
            act[:, pl.ds(pl.multiple_of(ATT + j * TILE, TILE), TILE)] = g.astype(jnp.bfloat16)
            issue(u + NBUF)
            return 0

        @pl.when(do_c)
        def _():
            lax.fori_loop(0, T_IN, in_tile, 0)

        @pl.when(do_rs)
        def _():
            remote(pbuf.at[po, pl.ds(half + 8 * (1 - a1), 8)], r1, RS1, p1).wait()
            add_rows(po, quarter + 4 * (1 - a2), r1, 4 * (1 - a2), 4)

        @pl.when(s >= 1)
        def _():
            pl.semaphore_wait(ready.at[2], 1)

        @pl.when(do_rs)
        def _():
            remote(pbuf.at[po, pl.ds(quarter + 4 * (1 - a2), 4)], r2, RS2, p2).start()
            add_rows(po, own, r1, 4 * a2, 4)

        def attend(step, _):
            seqs = [AT_STEP * step + k for k in range(AT_STEP)]
            curs = [cur_ref[c * GROUP + i] for i in seqs]

            def part(i, k):
                lo = qkv[2 * k, pl.ds(i, STEPS, stride=GROUP), :]
                hi = qkv[2 * k + 1, pl.ds(i, STEPS, stride=GROUP), :]
                return lo, hi

            def turn(lo, hi, cos_t, sin_t):
                other = jnp.where(even_lane, pltpu.roll(lo, 127, 1), pltpu.roll(lo, 1, 1))
                return jnp.concatenate([lo * cos_t + other * sin_t, hi], axis=1)

            def both(a, b):
                return jnp.concatenate([a, b], axis=0).astype(jnp.bfloat16)

            qs, ks, vs = [], [], []
            for i, cur in zip(seqs, curs):
                cos_t, sin_t = cos_ref[pl.ds(cur, STEPS), :], sin_ref[pl.ds(cur, STEPS), :]
                qs.append(both(*[turn(*part(i, k), cos_t, sin_t) for k in (0, 1)]))
                ks.append(both(*[turn(*part(i, k), cos_t, sin_t) for k in (2, 3)]))
                vs.append(both(*[jnp.concatenate(part(i, k), axis=1) for k in (4, 5)]))
            puts = [jnp.where(put_same & (put_off == cur), 1.0, 0.0).astype(jnp.bfloat16) for cur in curs]
            writ = [(wr_slot >= cur) & (wr_slot < cur + STEPS) for cur in curs]

            def merge(buf, new):
                olds = [buf[i].reshape(2 * SLOTS, HEAD).astype(jnp.float32) for i in seqs]
                put = [jnp.dot(p, n, preferred_element_type=jnp.float32) for p, n in zip(puts, new)]
                return [jnp.where(w, p, o).astype(jnp.bfloat16) for w, p, o in zip(writ, put, olds)]

            k_all, v_all = merge(kbuf, ks), merge(vbuf, vs)
            sc = [lax.dot_general(q, k, (((1,), (1,)), ((), ())), preferred_element_type=jnp.float32) * (HEAD ** -0.5) for q, k in zip(qs, k_all)]
            sc = [jnp.where(see_same & (see_off <= cur), x, -jnp.inf) for x, cur in zip(sc, curs)]
            ex = [jnp.exp(x - jnp.max(x, axis=-1, keepdims=True)) for x in sc]
            pr = [(e / jnp.sum(e, axis=-1, keepdims=True)).astype(jnp.bfloat16) for e in ex]
            cx = [jnp.dot(p, v, preferred_element_type=jnp.float32) for p, v in zip(pr, v_all)]
            for n, i in enumerate(seqs):
                kbuf[i] = k_all[n].reshape(SLOTS, HEADS, HEAD)
                vbuf[i] = v_all[n].reshape(SLOTS, HEADS, HEAD)
                for h in range(HEADS):
                    for w in range(2):
                        ctx[2 * h + w, pl.ds(i, STEPS, stride=GROUP), :] = cx[n][h * STEPS:(h + 1) * STEPS, w * 128:(w + 1) * 128]
            return 0

        def out_tile(j, _):
            u = s * T_ALL + T_QKV + T_IN + j
            b = u % NBUF
            pltpu.make_async_copy(win.at[0, pl.ds(0, ATT + FF), pl.ds(0, TILE)], wbuf.at[b, pl.ds(0, ATT + FF), :], wsem.at[b]).wait()
            acc = jnp.dot(act[...], wbuf[b, :ATT + FF, :], preferred_element_type=jnp.float32)
            pbuf[pn, :, :, pl.ds(pl.multiple_of(j * TILE, TILE), TILE)] = acc.astype(jnp.bfloat16).reshape(STEPS, GROUP, TILE)

            @pl.when(j >= 1)
            def _():
                send_half(j - 1)
            issue(u + NBUF)
            return 0

        def send_half(j):
            cols = pl.ds(pl.multiple_of(j * TILE, TILE), TILE)
            remote(pbuf.at[pn, pl.ds(16 - half, 16), :, cols], r0.at[:, :, cols], RS0, sib).start()

        @pl.when(do_c)
        def _():
            pltpu.make_async_copy(kc_hbm.at[0, pl.ds(0, GROUP)], kbuf, csem.at[0]).wait()
            pltpu.make_async_copy(vc_hbm.at[0, pl.ds(0, GROUP)], vbuf, csem.at[1]).wait()
            lax.fori_loop(0, GROUP // AT_STEP, attend, 0)
            pltpu.make_async_copy(kbuf, ko_hbm.at[layer, pl.ds(cseq, GROUP)], cosem.at[0]).start()
            pltpu.make_async_copy(vbuf, vo_hbm.at[layer, pl.ds(cseq, GROUP)], cosem.at[1]).start()
            for k in range(4):
                act[:, k * 128:(k + 1) * 128] = ctx[k].astype(jnp.bfloat16)

            @pl.when(s >= 1)
            def _():
                pl.semaphore_wait(r0free, 1)
            lax.fori_loop(0, OUT_SPLIT, out_tile, 0)

        @pl.when(do_rs)
        def _():
            remote(pbuf.at[po, pl.ds(quarter + 4 * (1 - a2), 4)], r2, RS2, p2).wait()

            @pl.when(l1 == 0)
            def _():
                pltpu.make_async_copy(x_hbm.at[pl.ds(0, 4), pl.ds(0, GROUP), :], xres.at[c1], xsem).wait()

            def finish(t, _):
                tot = pbuf[po, own + t].astype(jnp.float32) + r2[t].astype(jnp.float32)
                new = (xres[c1, t].astype(jnp.float32) + tot + bout_ref[l1]).astype(jnp.bfloat16)

                @pl.when(l1 == 0)
                def _():
                    xres[c1, t] = new
                    gbuf[gn, own + t] = norm_rows(new.astype(jnp.float32), gain_ref[1], bias_ref[1])

                @pl.when(l1 == 1)
                def _():
                    gbuf[gn, own + t] = new
                return 0
            for t in range(4):
                finish(t, 0)
            pl.semaphore_wait(gfree, 1)
            remote(gbuf.at[gn, pl.ds(own, 4)], gbuf.at[gn, pl.ds(own, 4)], AGA, p2).start()

        @pl.when(do_ag)
        def _():
            remote(gbuf.at[gb, pl.ds(quarter, 8)], gbuf.at[gb, pl.ds(quarter, 8)], AGB, p1).wait()

        @pl.when(s <= N_TASKS)
        def _():
            for k in (1, 2):
                pl.semaphore_signal(ready.at[k], inc=1, device_id={"tp": partners[k]}, device_id_type=MESH)

        @pl.when(s >= 1)
        def _():
            pl.semaphore_wait(ready.at[0], 1)

        @pl.when(do_ag)
        def _():
            remote(gbuf.at[gb, pl.ds(half, 16)], gbuf.at[gb, pl.ds(half, 16)], AGC, sib).start()

        @pl.when(do_c)
        def _():
            lax.fori_loop(OUT_SPLIT, T_OUT, out_tile, 0)
            send_half(T_OUT - 1)

        @pl.when(do_ag)
        def _():
            remote(gbuf.at[gb, pl.ds(half, 16)], gbuf.at[gb, pl.ds(half, 16)], AGC, sib).wait()
            pltpu.make_async_copy(gbuf.at[gb], out_hbm.at[:, pl.ds(pl.multiple_of(c2 * GROUP, GROUP), GROUP), :], gsem).start()

        @pl.when(s <= N_TASKS)
        def _():
            pl.semaphore_signal(ready.at[0], inc=1, device_id={"tp": sib}, device_id_type=MESH)
        return 0

    lax.fori_loop(0, N_TASKS + 2, slot, 0)
    pltpu.make_async_copy(gbuf.at[0], out_hbm.at[:, pl.ds(0, GROUP), :], gsem).wait()
    pltpu.make_async_copy(kbuf, ko_hbm.at[0, pl.ds(0, GROUP)], cosem.at[0]).wait()
    pltpu.make_async_copy(vbuf, vo_hbm.at[0, pl.ds(0, GROUP)], cosem.at[1]).wait()


def rotary_tables():
    lane = np.arange(128)
    inv_freq = np.float32(1) / np.power(np.float32(10000), (lane // 2 * 2).astype(np.float32) / np.float32(ROT_DIM))
    inv_freq = np.where(lane < ROT_DIM, inv_freq, 0).astype(np.float32)
    angles = np.arange(SLOTS, dtype=np.float32)[:, None] * inv_freq[None, :]
    sign = np.where(lane % 2 == 0, -1.0, 1.0)
    return np.cos(angles.astype(np.float64)).astype(np.float32), (np.sin(angles.astype(np.float64)) * sign).astype(np.float32)


def decode_shard(x_steps, cur_len, k_cache, v_cache, ln_gain, ln_bias, w_q, w_k, w_v, w_o, w_in, b_in, w_out, b_out):
    n_layers, batch, slots, heads, dim = k_cache.shape
    f32 = jnp.float32
    cos_tab, sin_tab = rotary_tables()
    flat = k_cache.shape
    bf = jnp.bfloat16
    any_spec, vmem = pl.BlockSpec(memory_space=pl.ANY), pl.BlockSpec(memory_space=pltpu.VMEM)
    out, k_out, v_out = pl.pallas_call(
        kernel,
        out_shape=(jax.ShapeDtypeStruct(x_steps.shape, bf), jax.ShapeDtypeStruct(flat, bf), jax.ShapeDtypeStruct(flat, bf)),
        in_specs=[pl.BlockSpec(memory_space=pltpu.SMEM), any_spec, any_spec, any_spec] + [vmem] * 6 + [any_spec] * 6,
        out_specs=(any_spec, any_spec, any_spec),
        scratch_shapes=[
            pltpu.VMEM((2, STEPS, GROUP, WIDTH), bf),
            pltpu.VMEM((2, STEPS, GROUP, WIDTH), bf),
            pltpu.VMEM((2, STEPS, GROUP, WIDTH), bf),
            pltpu.VMEM((16, GROUP, WIDTH), bf),
            pltpu.VMEM((8, GROUP, WIDTH), bf),
            pltpu.VMEM((4, GROUP, WIDTH), bf),
            pltpu.VMEM((N_GROUPS, 4, GROUP, WIDTH), bf),
            pltpu.VMEM((12, ROWS, 128), f32),
            pltpu.VMEM((4, ROWS, 128), f32),
            pltpu.VMEM((ROWS, ATT + FF), bf),
            pltpu.VMEM((NBUF, WIDTH, TILE), bf),
            pltpu.VMEM((GROUP, SLOTS, HEADS, HEAD), bf),
            pltpu.VMEM((GROUP, SLOTS, HEADS, HEAD), bf),
            pltpu.VMEM((N_LAYERS, 1, WIDTH), f32),
            pltpu.VMEM((N_LAYERS, 1, WIDTH), f32),
            pltpu.VMEM((N_LAYERS, 1, WIDTH), f32),
            pltpu.VMEM((N_LAYERS, T_IN, 1, TILE), f32),
            pltpu.SemaphoreType.DMA((NBUF,)),
            pltpu.SemaphoreType.DMA((2,)),
            pltpu.SemaphoreType.DMA((2,)),
            pltpu.SemaphoreType.DMA((2,)),
            pltpu.SemaphoreType.DMA,
            pltpu.SemaphoreType.DMA,
            pltpu.SemaphoreType.DMA((6,)),
            pltpu.SemaphoreType.DMA((6,)),
            pltpu.SemaphoreType.REGULAR((3,)),
            pltpu.SemaphoreType.REGULAR,
            pltpu.SemaphoreType.REGULAR,
        ],
        compiler_params=pltpu.CompilerParams(collective_id=0, has_side_effects=True, vmem_limit_bytes=62 * 1024 * 1024),
    )(cur_len, x_steps, k_cache.reshape(flat), v_cache.reshape(flat),
      ln_gain, ln_bias, b_out, b_in, cos_tab, sin_tab, w_q, w_k, w_v, w_o, w_in, w_out)
    return out, k_out.reshape(k_cache.shape), v_out.reshape(v_cache.shape)


def solution(mesh):
    cache_spec = P(None, "dp", None, "tp", None)
    in_specs = (P(None, "dp", None), P("dp"), cache_spec, cache_spec, P(None, None), P(None, None),
                P(None, None, "tp"), P(None, None, "tp"), P(None, None, "tp"), P(None, "tp", None),
                P(None, None, "tp"), P(None, "tp"), P(None, "tp", None), P(None, None))
    out_specs = (P(None, "dp", None), cache_spec, cache_spec)
    return jax.shard_map(decode_shard, mesh=mesh, in_specs=in_specs, out_specs=out_specs, check_vma=False)
```

```python
import functools

import jax
import jax.numpy as jnp
import numpy as np
from jax import lax
from jax.experimental import pallas as pl
from jax.experimental.pallas import tpu as pltpu
from jax.sharding import PartitionSpec as P

MESH = pl.DeviceIdType.MESH
ROT_DIM = 64
LN_EPS = 1e-5
GELU_C = 0.7978845608028654
WIDTH, HEAD, STEPS, SLOTS, HEADS = 4096, 256, 32, 64, 2
GROUP = 16
N_GROUPS, N_LAYERS = 4, 2
N_TASKS = N_GROUPS * N_LAYERS
ROWS = STEPS * GROUP
FF, ATT = 2048, 512
TILE = 512
T_QKV, T_IN, T_OUT = 3 * ATT // TILE, FF // TILE, WIDTH // TILE
T_ALL = T_QKV + T_IN + T_OUT
NBUF = 3
LN_STEP = 4
AT_STEP = 8
TOP_TILES, IN_SPLIT, OUT_SPLIT = 1, 3, 4
T_EARLY = 6
EARLY = T_EARLY * TILE
RS0, RS0_LATE, RS1, RS1_LATE, RS2, AGA, AGB, AGC = range(8)


def norm_rows(x, gain, bias):
    mean = jnp.mean(x, axis=-1, keepdims=True)
    centered = x - mean
    var = jnp.mean(centered * centered, axis=-1, keepdims=True)
    return (centered * lax.rsqrt(var + LN_EPS) * gain + bias).astype(jnp.bfloat16)


def kernel(cur_ref, x_hbm, kc_hbm, vc_hbm, gain_in, bias_in, bout_in, bin_in, cos_ref, sin_ref,
           wq, wk, wv, wo, win, wout, out_hbm, ko_hbm, vo_hbm,
           hbuf, gbuf, pbuf, r0, r1, r2, xres, qkv, ctx, act, wbuf, kbuf, vbuf, gain_ref, bias_ref, bout_ref, bin_ref,
           wsem, hsem, csem, cosem, xsem, gsem, ssem, rsem, ready, gfree):
    me = lax.axis_index("tp")
    core = me % 2
    xc = (me // 2) % 2
    yc = me // 4
    sib = me + 1 - 2 * core
    xn = me + 2 - 4 * xc
    yn = me + 4 - 8 * yc
    a1 = (1 - core) * xc + core * yc
    a2 = (1 - core) * yc + core * xc
    p1 = (1 - core) * xn + core * yn
    p2 = (1 - core) * yn + core * xn
    half = 16 * core
    quarter = half + 8 * a1
    own = quarter + 4 * a2
    partners = (sib, p1, p2)

    barrier = pltpu.get_barrier_semaphore()
    for dev in partners:
        pl.semaphore_signal(barrier, inc=1, device_id={"tp": dev}, device_id_type=MESH)
    pl.semaphore_wait(barrier, 3)

    def remote(src, dst, idx, dev):
        return pltpu.make_async_remote_copy(src_ref=src, dst_ref=dst, send_sem=ssem.at[idx], recv_sem=rsem.at[idx],
                                            device_id={"tp": dev}, device_id_type=MESH)

    def issue(u):
        @pl.when(u < N_TASKS * T_ALL)
        def _():
            task, j = u // T_ALL, u % T_ALL
            layer = task // N_GROUPS
            b = u % NBUF
            for k, ref in enumerate((wq, wk, wv)):
                n = ATT // TILE

                @pl.when((j >= n * k) & (j < n * k + n))
                def _():
                    col = pl.multiple_of((j - n * k) * TILE, TILE)
                    pltpu.make_async_copy(ref.at[layer, :, pl.ds(col, TILE)], wbuf.at[b], wsem.at[b]).start()

            @pl.when((j >= T_QKV) & (j < T_QKV + T_IN))
            def _():
                col = pl.multiple_of((j - T_QKV) * TILE, TILE)
                pltpu.make_async_copy(win.at[layer, :, pl.ds(col, TILE)], wbuf.at[b], wsem.at[b]).start()

            @pl.when(j >= T_QKV + T_IN)
            def _():
                col = pl.multiple_of((j - T_QKV - T_IN) * TILE, TILE)
                pltpu.make_async_copy(wo.at[layer, :, pl.ds(col, TILE)], wbuf.at[b, pl.ds(0, ATT), :], wsem.at[b]).start()
                pltpu.make_async_copy(wout.at[layer, :, pl.ds(col, TILE)], wbuf.at[b, pl.ds(ATT, FF), :], wsem.at[b]).start()

    def load_h(task):
        c = task % N_GROUPS
        b = task % 2
        cols = pl.ds(pl.multiple_of(c * GROUP, GROUP), GROUP)

        @pl.when(task < N_GROUPS)
        def _():
            pltpu.make_async_copy(x_hbm.at[:, cols, :], hbuf.at[b], hsem.at[b]).start()

        @pl.when((task >= N_GROUPS) & (task < N_TASKS))
        def _():
            pltpu.make_async_copy(out_hbm.at[:, cols, :], hbuf.at[b], hsem.at[b]).start()

    def add_rows(p, base, terms, n, cols):
        def body(t, _):
            for k in range(2):
                total = pbuf[p, base + 2 * t + k, :, cols].astype(jnp.float32)
                for ref, start in terms:
                    total = total + ref[start + 2 * t + k, :, cols].astype(jnp.float32)
                pbuf[p, base + 2 * t + k, :, cols] = total.astype(jnp.bfloat16)
            return 0
        lax.fori_loop(0, n // 2, body, 0)

    early, late = pl.ds(0, EARLY), pl.ds(EARLY, WIDTH - EARLY)
    away1 = half + 8 * (1 - a1)
    away2 = quarter + 4 * (1 - a2)

    def start_exchange(p, cols, idx0, idx1):
        remote(pbuf.at[p, pl.ds(16 - half, 16), :, cols], r0.at[p, :, :, cols], idx0, sib).wait()
        add_rows(p, away1, [(r0.at[p], 8 * (1 - a1))], 8, cols)
        remote(pbuf.at[p, pl.ds(away1, 8), :, cols], r1.at[:, :, cols], idx1, p1).start()

    for u in range(NBUF):
        issue(u)
    load_h(0)
    for l in range(N_LAYERS):
        for dst, src in ((gain_ref, gain_in), (bias_ref, bias_in), (bout_ref, bout_in)):
            dst[l] = src[l:l + 1, :].astype(jnp.float32)
        for j in range(T_IN):
            bin_ref[l, j] = bin_in[l:l + 1, j * TILE:(j + 1) * TILE].astype(jnp.float32)

    row_i = lax.broadcasted_iota(jnp.int32, (2 * SLOTS, 2 * STEPS), 0)
    col_i = lax.broadcasted_iota(jnp.int32, (2 * SLOTS, 2 * STEPS), 1)
    put_same = (row_i % 2) == (col_i // STEPS)
    put_off = row_i // 2 - col_i % STEPS
    wr_slot = lax.broadcasted_iota(jnp.int32, (2 * SLOTS, HEAD), 0) // 2
    s_row = lax.broadcasted_iota(jnp.int32, (2 * STEPS, 2 * SLOTS), 0)
    s_col = lax.broadcasted_iota(jnp.int32, (2 * STEPS, 2 * SLOTS), 1)
    see_same = (s_row // STEPS) == (s_col % 2)
    see_off = s_col // 2 - s_row % STEPS
    even_lane = lax.broadcasted_iota(jnp.int32, (STEPS, 128), 1) % 2 == 0

    def slot(s, _):
        pn, po = s % 2, (s + 1) % 2
        gb, gn = s % 2, (s + 1) % 2
        hb = s % 2
        layer, c = s // N_GROUPS, s % N_GROUPS
        l1, c1 = (s + N_GROUPS - 1) // N_GROUPS - 1, (s + N_GROUPS - 1) % N_GROUPS
        c2 = (s + N_GROUPS - 2) % N_GROUPS
        do_c = s < N_TASKS
        do_rs = (s >= 1) & (s <= N_TASKS)
        do_ag = s >= 2
        cseq = pl.multiple_of(c * GROUP, GROUP)

        def mm1_tile(j):
            u = s * T_ALL + j
            b = u % NBUF
            pltpu.make_async_copy(win.at[0, :, pl.ds(0, TILE)], wbuf.at[b], wsem.at[b]).wait()
            acc = jnp.dot(hbuf[hb].reshape(ROWS, WIDTH), wbuf[b], preferred_element_type=jnp.float32)
            return acc, u

        def qkv_tile(j, _):
            acc, u = mm1_tile(j)
            for w in range(TILE // 128):
                qkv[TILE // 128 * j + w] = acc[:, w * 128:(w + 1) * 128]
            issue(u + NBUF)
            return 0

        @pl.when(do_c)
        def _():
            @pl.when(s >= 1)
            def _():
                pltpu.make_async_copy(kbuf, ko_hbm.at[0, pl.ds(0, GROUP)], cosem.at[0]).wait()
                pltpu.make_async_copy(vbuf, vo_hbm.at[0, pl.ds(0, GROUP)], cosem.at[1]).wait()
            pltpu.make_async_copy(kc_hbm.at[layer, pl.ds(cseq, GROUP)], kbuf, csem.at[0]).start()
            pltpu.make_async_copy(vc_hbm.at[layer, pl.ds(cseq, GROUP)], vbuf, csem.at[1]).start()
            pltpu.make_async_copy(x_hbm.at[:, pl.ds(0, GROUP), :], hbuf.at[hb], hsem.at[hb]).wait()

            @pl.when(layer == 0)
            def _():
                def ln(t, _):
                    done = [norm_rows(hbuf[hb, LN_STEP * t + k].astype(jnp.float32), gain_ref[0], bias_ref[0]) for k in range(LN_STEP)]
                    for k in range(LN_STEP):
                        hbuf[hb, LN_STEP * t + k] = done[k]
                    return 0
                lax.fori_loop(0, STEPS // LN_STEP, ln, 0)

            lax.fori_loop(0, TOP_TILES, qkv_tile, 0)

        @pl.when(do_rs)
        def _():
            start_exchange(po, late, RS0_LATE, RS1_LATE)

        @pl.when(s >= 1)
        def _():
            pl.semaphore_signal(ready.at[0], inc=1, device_id={"tp": sib}, device_id_type=MESH)

        @pl.when(do_ag)
        def _():
            remote(gbuf.at[gb, pl.ds(own, 4)], gbuf.at[gb, pl.ds(own, 4)], AGA, p2).wait()
            remote(gbuf.at[gb, pl.ds(quarter, 8)], gbuf.at[gb, pl.ds(quarter, 8)], AGB, p1).start()

        @pl.when(do_c)
        def _():
            lax.fori_loop(TOP_TILES, T_QKV, qkv_tile, 0)

        @pl.when(s >= 3)
        def _():
            pltpu.make_async_copy(gbuf.at[gn], out_hbm.at[:, pl.ds(0, GROUP), :], gsem).wait()

        @pl.when(do_rs)
        def _():
            pl.semaphore_signal(gfree, inc=1, device_id={"tp": p2}, device_id_type=MESH)

        load_h(s + 1)

        @pl.when(do_rs & (l1 == 0))
        def _():
            pltpu.make_async_copy(x_hbm.at[pl.ds(own, 4), pl.ds(pl.multiple_of(c1 * GROUP, GROUP), GROUP), :], xres.at[c1], xsem).start()

        def in_tile(j, _):
            acc, u = mm1_tile(T_QKV + j)
            y = acc + bin_ref[layer, j]
            g = 0.5 * y * (1.0 + jnp.tanh(GELU_C * (y + 0.044715 * y * y * y)))
            act[:, pl.ds(pl.multiple_of(ATT + j * TILE, TILE), TILE)] = g.astype(jnp.bfloat16)
            issue(u + NBUF)
            return 0

        @pl.when(do_c)
        def _():
            lax.fori_loop(0, IN_SPLIT, in_tile, 0)

        @pl.when(s >= 1)
        def _():
            pl.semaphore_wait(ready.at[2], 1)

        @pl.when(do_rs)
        def _():
            for cols, idx in ((early, RS1), (late, RS1_LATE)):
                remote(pbuf.at[po, pl.ds(away1, 8), :, cols], r1.at[:, :, cols], idx, p1).wait()
            add_rows(po, away2, [(r0.at[po], 8 * a1 + 4 * (1 - a2)), (r1, 4 * (1 - a2))], 4, pl.ds(0, WIDTH))
            remote(pbuf.at[po, pl.ds(away2, 4)], r2, RS2, p2).start()

        @pl.when(do_c)
        def _():
            lax.fori_loop(IN_SPLIT, T_IN, in_tile, 0)

        def attend(step, _):
            seqs = [AT_STEP * step + k for k in range(AT_STEP)]
            curs = [cur_ref[c * GROUP + i] for i in seqs]

            def part(i, k):
                lo = qkv[2 * k, pl.ds(i, STEPS, stride=GROUP), :]
                hi = qkv[2 * k + 1, pl.ds(i, STEPS, stride=GROUP), :]
                return lo, hi

            def turn(lo, hi, cos_t, sin_t):
                other = jnp.where(even_lane, pltpu.roll(lo, 127, 1), pltpu.roll(lo, 1, 1))
                return jnp.concatenate([lo * cos_t + other * sin_t, hi], axis=1)

            def both(a, b):
                return jnp.concatenate([a, b], axis=0).astype(jnp.bfloat16)

            qs, ks, vs = [], [], []
            for i, cur in zip(seqs, curs):
                cos_t, sin_t = cos_ref[pl.ds(cur, STEPS), :], sin_ref[pl.ds(cur, STEPS), :]
                qs.append(both(*[turn(*part(i, k), cos_t, sin_t) for k in (0, 1)]))
                ks.append(both(*[turn(*part(i, k), cos_t, sin_t) for k in (2, 3)]))
                vs.append(both(*[jnp.concatenate(part(i, k), axis=1) for k in (4, 5)]))
            puts = [jnp.where(put_same & (put_off == cur), 1.0, 0.0).astype(jnp.bfloat16) for cur in curs]
            writ = [(wr_slot >= cur) & (wr_slot < cur + STEPS) for cur in curs]

            def merge(buf, new):
                olds = [buf[i].reshape(2 * SLOTS, HEAD).astype(jnp.float32) for i in seqs]
                put = [jnp.dot(p, n, preferred_element_type=jnp.float32) for p, n in zip(puts, new)]
                return [jnp.where(w, p, o).astype(jnp.bfloat16) for w, p, o in zip(writ, put, olds)]

            k_all, v_all = merge(kbuf, ks), merge(vbuf, vs)
            sc = [lax.dot_general(q, k, (((1,), (1,)), ((), ())), preferred_element_type=jnp.float32) * (HEAD ** -0.5) for q, k in zip(qs, k_all)]
            sc = [jnp.where(see_same & (see_off <= cur), x, -jnp.inf) for x, cur in zip(sc, curs)]
            ex = [jnp.exp(x - jnp.max(x, axis=-1, keepdims=True)) for x in sc]
            pr = [(e / jnp.sum(e, axis=-1, keepdims=True)).astype(jnp.bfloat16) for e in ex]
            cx = [jnp.dot(p, v, preferred_element_type=jnp.float32) for p, v in zip(pr, v_all)]
            for n, i in enumerate(seqs):
                kbuf[i] = k_all[n].reshape(SLOTS, HEADS, HEAD)
                vbuf[i] = v_all[n].reshape(SLOTS, HEADS, HEAD)
                for h in range(HEADS):
                    for w in range(2):
                        ctx[2 * h + w, pl.ds(i, STEPS, stride=GROUP), :] = cx[n][h * STEPS:(h + 1) * STEPS, w * 128:(w + 1) * 128]
            return 0

        def out_tile(j, _):
            u = s * T_ALL + T_QKV + T_IN + j
            b = u % NBUF
            pltpu.make_async_copy(win.at[0, pl.ds(0, ATT + FF), pl.ds(0, TILE)], wbuf.at[b, pl.ds(0, ATT + FF), :], wsem.at[b]).wait()
            acc = jnp.dot(act[...], wbuf[b, :ATT + FF, :], preferred_element_type=jnp.float32)
            pbuf[pn, :, :, pl.ds(pl.multiple_of(j * TILE, TILE), TILE)] = acc.astype(jnp.bfloat16).reshape(STEPS, GROUP, TILE)

            @pl.when(j >= 1)
            def _():
                send_half(j - 1)
            issue(u + NBUF)
            return 0

        def send_half(j):
            cols = pl.ds(pl.multiple_of(j * TILE, TILE), TILE)
            remote(pbuf.at[pn, pl.ds(16 - half, 16), :, cols], r0.at[pn, :, :, cols], RS0 + j // T_EARLY, sib).start()

        @pl.when(do_c)
        def _():
            pltpu.make_async_copy(kc_hbm.at[0, pl.ds(0, GROUP)], kbuf, csem.at[0]).wait()
            pltpu.make_async_copy(vc_hbm.at[0, pl.ds(0, GROUP)], vbuf, csem.at[1]).wait()
            lax.fori_loop(0, GROUP // AT_STEP, attend, 0)
            pltpu.make_async_copy(kbuf, ko_hbm.at[layer, pl.ds(cseq, GROUP)], cosem.at[0]).start()
            pltpu.make_async_copy(vbuf, vo_hbm.at[layer, pl.ds(cseq, GROUP)], cosem.at[1]).start()
            for k in range(4):
                act[:, k * 128:(k + 1) * 128] = ctx[k].astype(jnp.bfloat16)

        @pl.when(s >= 1)
        def _():
            pl.semaphore_wait(ready.at[0], 1)

        @pl.when(do_c)
        def _():
            lax.fori_loop(0, OUT_SPLIT, out_tile, 0)

        @pl.when(do_rs)
        def _():
            remote(pbuf.at[po, pl.ds(away2, 4)], r2, RS2, p2).wait()

            @pl.when(l1 == 0)
            def _():
                pltpu.make_async_copy(x_hbm.at[pl.ds(0, 4), pl.ds(0, GROUP), :], xres.at[c1], xsem).wait()

            def finish(t, _):
                tot = pbuf[po, own + t].astype(jnp.float32) + r0[po, 8 * a1 + 4 * a2 + t].astype(jnp.float32)
                tot = tot + r1[4 * a2 + t].astype(jnp.float32) + r2[t].astype(jnp.float32)
                new = (xres[c1, t].astype(jnp.float32) + tot + bout_ref[l1]).astype(jnp.bfloat16)

                @pl.when(l1 == 0)
                def _():
                    xres[c1, t] = new
                    gbuf[gn, own + t] = norm_rows(new.astype(jnp.float32), gain_ref[1], bias_ref[1])

                @pl.when(l1 == 1)
                def _():
                    gbuf[gn, own + t] = new
                return 0
            for t in range(4):
                finish(t, 0)
            pl.semaphore_wait(gfree, 1)
            remote(gbuf.at[gn, pl.ds(own, 4)], gbuf.at[gn, pl.ds(own, 4)], AGA, p2).start()

        @pl.when(do_ag)
        def _():
            remote(gbuf.at[gb, pl.ds(quarter, 8)], gbuf.at[gb, pl.ds(quarter, 8)], AGB, p1).wait()

        @pl.when(s <= N_TASKS)
        def _():
            for k in (1, 2):
                pl.semaphore_signal(ready.at[k], inc=1, device_id={"tp": partners[k]}, device_id_type=MESH)

        @pl.when(do_ag)
        def _():
            remote(gbuf.at[gb, pl.ds(half, 16)], gbuf.at[gb, pl.ds(half, 16)], AGC, sib).start()

        @pl.when(do_c)
        def _():
            lax.fori_loop(OUT_SPLIT, T_OUT, out_tile, 0)
            send_half(T_OUT - 1)

        @pl.when(s <= N_TASKS)
        def _():
            pl.semaphore_wait(ready.at[1], 1)

        @pl.when(do_c)
        def _():
            start_exchange(pn, early, RS0, RS1)

        @pl.when(do_ag)
        def _():
            remote(gbuf.at[gb, pl.ds(half, 16)], gbuf.at[gb, pl.ds(half, 16)], AGC, sib).wait()
            pltpu.make_async_copy(gbuf.at[gb], out_hbm.at[:, pl.ds(pl.multiple_of(c2 * GROUP, GROUP), GROUP), :], gsem).start()
        return 0

    lax.fori_loop(0, N_TASKS + 2, slot, 0)
    pltpu.make_async_copy(gbuf.at[0], out_hbm.at[:, pl.ds(0, GROUP), :], gsem).wait()
    pltpu.make_async_copy(kbuf, ko_hbm.at[0, pl.ds(0, GROUP)], cosem.at[0]).wait()
    pltpu.make_async_copy(vbuf, vo_hbm.at[0, pl.ds(0, GROUP)], cosem.at[1]).wait()


def rotary_tables():
    lane = np.arange(128)
    inv_freq = np.float32(1) / np.power(np.float32(10000), (lane // 2 * 2).astype(np.float32) / np.float32(ROT_DIM))
    inv_freq = np.where(lane < ROT_DIM, inv_freq, 0).astype(np.float32)
    angles = np.arange(SLOTS, dtype=np.float32)[:, None] * inv_freq[None, :]
    sign = np.where(lane % 2 == 0, -1.0, 1.0)
    return np.cos(angles.astype(np.float64)).astype(np.float32), (np.sin(angles.astype(np.float64)) * sign).astype(np.float32)


def decode_shard(x_steps, cur_len, k_cache, v_cache, ln_gain, ln_bias, w_q, w_k, w_v, w_o, w_in, b_in, w_out, b_out):
    n_layers, batch, slots, heads, dim = k_cache.shape
    f32 = jnp.float32
    cos_tab, sin_tab = rotary_tables()
    flat = k_cache.shape
    bf = jnp.bfloat16
    any_spec, vmem = pl.BlockSpec(memory_space=pl.ANY), pl.BlockSpec(memory_space=pltpu.VMEM)
    out, k_out, v_out = pl.pallas_call(
        kernel,
        out_shape=(jax.ShapeDtypeStruct(x_steps.shape, bf), jax.ShapeDtypeStruct(flat, bf), jax.ShapeDtypeStruct(flat, bf)),
        in_specs=[pl.BlockSpec(memory_space=pltpu.SMEM), any_spec, any_spec, any_spec] + [vmem] * 6 + [any_spec] * 6,
        out_specs=(any_spec, any_spec, any_spec),
        scratch_shapes=[
            pltpu.VMEM((2, STEPS, GROUP, WIDTH), bf),
            pltpu.VMEM((2, STEPS, GROUP, WIDTH), bf),
            pltpu.VMEM((2, STEPS, GROUP, WIDTH), bf),
            pltpu.VMEM((2, 16, GROUP, WIDTH), bf),
            pltpu.VMEM((8, GROUP, WIDTH), bf),
            pltpu.VMEM((4, GROUP, WIDTH), bf),
            pltpu.VMEM((N_GROUPS, 4, GROUP, WIDTH), bf),
            pltpu.VMEM((12, ROWS, 128), f32),
            pltpu.VMEM((4, ROWS, 128), f32),
            pltpu.VMEM((ROWS, ATT + FF), bf),
            pltpu.VMEM((NBUF, WIDTH, TILE), bf),
            pltpu.VMEM((GROUP, SLOTS, HEADS, HEAD), bf),
            pltpu.VMEM((GROUP, SLOTS, HEADS, HEAD), bf),
            pltpu.VMEM((N_LAYERS, 1, WIDTH), f32),
            pltpu.VMEM((N_LAYERS, 1, WIDTH), f32),
            pltpu.VMEM((N_LAYERS, 1, WIDTH), f32),
            pltpu.VMEM((N_LAYERS, T_IN, 1, TILE), f32),
            pltpu.SemaphoreType.DMA((NBUF,)),
            pltpu.SemaphoreType.DMA((2,)),
            pltpu.SemaphoreType.DMA((2,)),
            pltpu.SemaphoreType.DMA((2,)),
            pltpu.SemaphoreType.DMA,
            pltpu.SemaphoreType.DMA,
            pltpu.SemaphoreType.DMA((8,)),
            pltpu.SemaphoreType.DMA((8,)),
            pltpu.SemaphoreType.REGULAR((3,)),
            pltpu.SemaphoreType.REGULAR,
        ],
        compiler_params=pltpu.CompilerParams(collective_id=0, has_side_effects=True, vmem_limit_bytes=62 * 1024 * 1024),
    )(cur_len, x_steps, k_cache.reshape(flat), v_cache.reshape(flat),
      ln_gain, ln_bias, b_out, b_in, cos_tab, sin_tab, w_q, w_k, w_v, w_o, w_in, w_out)
    return out, k_out.reshape(k_cache.shape), v_out.reshape(v_cache.shape)


def solution(mesh):
    cache_spec = P(None, "dp", None, "tp", None)
    in_specs = (P(None, "dp", None), P("dp"), cache_spec, cache_spec, P(None, None), P(None, None),
                P(None, None, "tp"), P(None, None, "tp"), P(None, None, "tp"), P(None, "tp", None),
                P(None, None, "tp"), P(None, "tp"), P(None, "tp", None), P(None, None))
    out_specs = (P(None, "dp", None), cache_spec, cache_spec)
    return jax.shard_map(decode_shard, mesh=mesh, in_specs=in_specs, out_specs=out_specs, check_vma=False)
```
